64 devices in a mesh: dp: 4 (over x, y), sp: 16 (over z, core).
Axes of the slice: x: 2, y: 2, z: 8, core: 2. Of those that a mesh axis runs over, the one named last changes fastest.
The devices are a block of a 4x4x8 slice.
Arguments:
- x: bfloat16 [16384, 5120], P(('dp', 'sp')), parts along dimension 0
- gain: bfloat16 [5120], replicated
- wq: bfloat16 [5120, 4096], replicated
- wk: bfloat16 [5120, 1024], replicated
- wv: bfloat16 [5120, 1024], replicated
- wo: bfloat16 [4096, 5120], replicated
Outputs:
- output: bfloat16 [16384, 5120], P(('dp', 'sp')), parts along dimension 0
There are 4 independent parts. The reference program is written for one: setup_inputs(seed, part) draws one part's arguments, and reference() takes and returns one part's arrays. A program takes and returns all parts, laid end to end along the dimension named above; an argument that names none is the same for every part.
All inputs are finite; a program needn't handle non-finite values.
Results may differ from the reference program's by a relative error of at most 0.012.
Values are sent between devices in bfloat16 or wider.
A program may use at most 768 MiB of HBM per device.

```python
import jax
import jax.numpy as jnp
from jax import lax

ROWS = 4096
D = 5120
HEADS = 32
KV_HEADS = 8
HEAD = 128
THETA = 10000


def setup_inputs(seed: int = 0, part: int = 0) -> dict:
    kx, kn, kq, kk, kv, ko = jax.random.split(jax.random.key(seed), 6)

    def weights(key, rows, columns):
        return jax.random.normal(key, (rows, columns), jnp.float32) * rows**-0.5

    drawn = {
        "x": jax.random.normal(jax.random.fold_in(kx, part), (ROWS, D), jnp.float32),
        "gain": 1 + 0.1 * jax.random.normal(kn, (D,), jnp.float32),
        "wq": 2 * weights(kq, D, HEADS * HEAD),
        "wk": 2 * weights(kk, D, KV_HEADS * HEAD),
        "wv": 4 * weights(kv, D, KV_HEADS * HEAD),
        "wo": weights(ko, HEADS * HEAD, D),
    }
    return {k: v.astype(jnp.bfloat16) for k, v in drawn.items()}


def normed(x, gain):
    wide = x.astype(jnp.float32)
    scale = lax.rsqrt(jnp.mean(wide * wide, -1, keepdims=True) + 1e-6)
    return (wide * scale * gain.astype(jnp.float32)).astype(jnp.bfloat16)


def turned(t, place, theta):
    half = t.shape[-1] // 2
    angle = place.astype(jnp.float32)[:, None] * theta ** (-jnp.arange(half, dtype=jnp.float32) / half)
    cos, sin = jnp.cos(angle)[:, None], jnp.sin(angle)[:, None]
    a, b = t[..., :half].astype(jnp.float32), t[..., half:].astype(jnp.float32)
    return jnp.concatenate([a * cos - b * sin, b * cos + a * sin], -1).astype(jnp.bfloat16)


def matmul(a, w):
    return jnp.dot(a, w, preferred_element_type=jnp.float32).astype(jnp.bfloat16)


def einsum(form, a, b):
    return jnp.einsum(form, a.astype(jnp.float32), b.astype(jnp.float32))


def attention(q, k, v):
    scores = einsum("tgsd,ugd->gstu", q, k) * q.shape[-1] ** -0.5
    token = jnp.arange(q.shape[0])
    scores = jnp.where(token[:, None] >= token, scores, -jnp.inf)
    weights = jax.nn.softmax(scores, -1).astype(jnp.bfloat16)
    return einsum("gstu,ugd->tgsd", weights, v).astype(jnp.bfloat16)


def reference(x, gain, wq, wk, wv, wo):
    a, place = normed(x, gain), jnp.arange(ROWS)
    q = turned(matmul(a, wq).reshape(ROWS, HEADS, HEAD), place, THETA).reshape(ROWS, KV_HEADS, -1, HEAD)
    k = turned(matmul(a, wk).reshape(ROWS, KV_HEADS, HEAD), place, THETA)
    v = matmul(a, wv).reshape(ROWS, KV_HEADS, HEAD)
    seen = attention(q, k, v).reshape(ROWS, HEADS * HEAD)
    return (x.astype(jnp.float32) + jnp.dot(seen, wo, preferred_element_type=jnp.float32)).astype(jnp.bfloat16)
```

```python
import functools

import jax
import jax.numpy as jnp
from jax import lax
from jax.experimental import pallas as pl
from jax.experimental.pallas import tpu as pltpu
from jax.sharding import PartitionSpec as P

HEAD = 128
THETA = 10000
HIDDEN = -2e30
LOG2E = 1.4426950408889634
CORES = 2
MESH = pl.DeviceIdType.MESH


def dot(a, b, ca=1, cb=0):
    return lax.dot_general(a, b, (((ca,), (cb,)), ((), ())), preferred_element_type=jnp.float32)


def kernel(x_hbm, gain_ref, cos_ref, sin_ref, wq, wk, wv, wo, y_hbm, xs, a, kv, qs, mix, tops, colkv, colq, rows, acc,
           load, fsend, frecv, bsend, brecv, ssend, srecv, *, chips, kvh, group):
    me = lax.axis_index("sp")
    z, c = lax.div(me, CORES), lax.rem(me, CORES)
    tok, depth = xs.shape
    wide = group * HEAD
    cols = group * tok
    far = chips // 2
    e2 = HEAD**-0.5 * LOG2E
    fmax = jnp.where(c == 0, far, far - 1)
    bmax = chips - 1 - fmax
    after = lax.rem(z + 1, chips) * CORES + c
    before = lax.rem(z + chips - 1, chips) * CORES + c
    other = z * CORES + 1 - c

    barrier = pltpu.get_barrier_semaphore()
    for peer in (after, before, other):
        pl.semaphore_signal(barrier, inc=1, device_id={"sp": peer}, device_id_type=MESH)

    x_load = pltpu.make_async_copy(x_hbm, xs, load.at[0])

    def kv_load(pair):
        at = pl.ds(pl.multiple_of(pair * 2 * HEAD, 2 * HEAD), 2 * HEAD)
        return (pltpu.make_async_copy(wk.at[:, at], colkv.at[:, pl.ds(0, 2 * HEAD)], load.at[1]),
                pltpu.make_async_copy(wv.at[:, at], colkv.at[:, pl.ds(2 * HEAD, 2 * HEAD)], load.at[2]))

    def q_load(h):
        return pltpu.make_async_copy(wq.at[:, pl.ds(pl.multiple_of(h * wide, wide), wide)], colq, load.at[3])

    def o_load(h):
        return pltpu.make_async_copy(wo.at[pl.ds(pl.multiple_of(h * wide, wide), wide), :], rows, load.at[4])

    x_load.start()
    for copy in kv_load(0):
        copy.start()
    q_load(0).start()
    o_load(0).start()

    def forward(h, chip, hop):
        piece = kv.at[h, chip * CORES + c]
        return pltpu.make_async_remote_copy(piece, piece, fsend.at[h, hop], frecv.at[h, hop], device_id={"sp": after}, device_id_type=MESH)

    def backward(h, chip, hop):
        piece = kv.at[h, chip * CORES + c]
        return pltpu.make_async_remote_copy(piece, piece, bsend.at[h, hop], brecv.at[h, hop], device_id={"sp": before}, device_id_type=MESH)

    def share(h, chip, core, way):
        piece = kv.at[h, chip * CORES + core]
        return pltpu.make_async_remote_copy(piece, piece, ssend.at[h, way], srecv.at[h, way], device_id={"sp": other}, device_id_type=MESH)

    def goes_forward(chip, hop):
        return (chip >= 0) & (chip + hop + 1 < chips) & (hop + 1 <= fmax)

    def goes_backward(chip, hop):
        return (chip < bmax) & (hop + 1 <= bmax)

    x_load.wait()

    def norm(i, _):
        at = pl.ds(pl.multiple_of(i * 16, 16), 16)
        t = xs[at, :].astype(jnp.float32)
        acc[at, :] = t
        scale = lax.rsqrt(jnp.mean(t * t, -1, keepdims=True) + 1e-6)
        a[at, :] = (t * scale * gain_ref[...].astype(jnp.float32)).astype(a.dtype)

    lax.fori_loop(0, tok // 16, norm, None)

    def turned(t):
        t = t.astype(jnp.bfloat16).astype(jnp.float32)
        return (t * cos_ref[...] + pltpu.roll(t, HEAD // 2, 1) * sin_ref[...]).astype(jnp.bfloat16)

    def project_kv(pair):
        for copy in kv_load(pair):
            copy.wait()
        k = dot(a[...], colkv[:, : 2 * HEAD])
        v = dot(a[...], colkv[:, 2 * HEAD :])
        for i in range(2):
            h = 2 * pair + i
            kv[h, me, :tok, :] = turned(k[:, i * HEAD : (i + 1) * HEAD])
            vt = v[:, i * HEAD : (i + 1) * HEAD].astype(jnp.bfloat16).T
            for n in range(tok // HEAD):
                kv[h, me, tok + n * HEAD : tok + (n + 1) * HEAD, :] = vt[:, n * HEAD : (n + 1) * HEAD]

        @pl.when(pair + 1 < kvh // 2)
        def _():
            for copy in kv_load(pair + 1):
                copy.start()

    def project_q(h):
        q_load(h).wait()
        t = dot(a[...], colq[...])
        for n in range(group):
            qs[h, n * tok : (n + 1) * tok, :] = turned(t[:, n * HEAD : (n + 1) * HEAD])

        @pl.when(h + 1 < kvh)
        def _():
            q_load(h + 1).start()

    strip = 256

    def attend(h, chip, first):
        k = kv[h, pl.ds(chip * CORES, CORES), :tok, :].reshape(CORES * tok, HEAD)
        vt = jnp.concatenate([kv[h, chip * CORES + i, tok + n * HEAD : tok + (n + 1) * HEAD, :] for i in range(CORES) for n in range(tok // HEAD)], axis=1)
        vt = jnp.concatenate([vt, jnp.ones((8, CORES * tok), vt.dtype)], axis=0)
        strips = range(0, cols, strip)
        scores = [dot(k, qs[h, at : at + strip, :], 1, 1) for at in strips]
        weights, keeps = [], []
        for at, s in zip(strips, scores):
            if first:
                key = lax.broadcasted_iota(jnp.int32, s.shape, 0)
                query = lax.rem(lax.broadcasted_iota(jnp.int32, s.shape, 1) + at, tok) + c * tok
                s = jnp.where(key <= query, s, HIDDEN)
                top = s.max(axis=0, keepdims=True)
            else:
                old = tops[h, :, at : at + strip]
                top = jnp.maximum(old, s.max(axis=0, keepdims=True))
                keeps.append(jnp.exp2((old - top) * e2))
            tops[h, :, at : at + strip] = top
            weights.append(jnp.exp2((s - top) * e2).astype(jnp.bfloat16))
        for n, at in enumerate(strips):
            new = dot(vt, weights[n])
            mix[h, :, at : at + strip] = new if first else mix[h, :, at : at + strip] * keeps[n] + new

    def finish(h):
        o_load(h).wait()
        parts = []
        for n in range(group):
            at = slice(n * tok, (n + 1) * tok)
            parts.append((mix[h, :HEAD, at] * (1 / mix[h, HEAD : HEAD + 1, at])).astype(jnp.bfloat16).T)
        seen = jnp.concatenate(parts, axis=1)
        step = 1024

        def out(i, _):
            at = pl.ds(pl.multiple_of(i * step, step), step)
            acc[:, at] += dot(seen, rows[:, at])

        lax.fori_loop(0, depth // step, out, None)

        @pl.when(h + 1 < kvh)
        def _():
            o_load(h + 1).start()

    def send_own(h):
        @pl.when(goes_forward(z, 0))
        def _():
            forward(h, z, 0).start()

        @pl.when(goes_backward(z, 0))
        def _():
            backward(h, z, 0).start()

        share(h, z, c, 0).start()

    def receive(h, e):
        chip = z - e

        @pl.when((chip >= 0) & (e <= fmax))
        def _():
            forward(h, chip, e - 1).wait_recv()

            @pl.when(goes_forward(chip, e))
            def _():
                forward(h, chip, e).start()

            share(h, chip, c, e).start()

        chip2 = lax.rem(z + e, chips)

        @pl.when((chip2 < bmax) & (e <= bmax))
        def _():
            backward(h, chip2, e - 1).wait_recv()

            @pl.when(goes_backward(chip2, e))
            def _():
                backward(h, chip2, e).start()

            @pl.when(z + e >= chips)
            def _():
                share(h, chip2, c, far + e).start()

    project_kv(0)
    pl.semaphore_wait(barrier, 3)
    send_own(0)
    project_q(0)

    def round_(t, _):
        @pl.when(t + 1 < kvh)
        def _():
            send_own(t + 1)

        for e in range(1, far + 1):
            @pl.when((t >= e) & (t - e < kvh))
            def _():
                receive(t - e, e)

        @pl.when(t < kvh)
        def _():
            share(t, z, 1 - c, 0).wait_recv()
            attend(t, z, True)

        @pl.when((lax.rem(t, 2) == 0) & (t + 2 < kvh))
        def _():
            project_kv(lax.div(t, 2) + 1)

        def piece(j, _):
            e = lax.div(j, 2) + 1
            back = lax.rem(j, 2)
            h = t - e
            chip = jnp.where(back == 1, z + e - chips, z - e)

            @pl.when((h >= 0) & (h < kvh) & (chip >= 0))
            def _():
                way = jnp.where(e == far, jnp.where(c == 0, 2 * far, far), e + back * far)
                share(h, chip, 1 - c, way).wait_recv()
                attend(h, chip, False)

        lax.fori_loop(0, 2 * far - 1, piece, None)

        @pl.when(t + 1 < kvh)
        def _():
            project_q(t + 1)

        @pl.when(t >= far)
        def _():
            finish(t - far)

    lax.fori_loop(0, kvh + far, round_, None)

    def drain(h, _):
        share(h, z, c, 0).wait_send()
        for hop in range(far):
            chip = z - hop

            @pl.when(goes_forward(chip, hop))
            def _():
                forward(h, chip, hop).wait_send()

            chip2 = lax.rem(z + hop, chips)

            @pl.when(goes_backward(chip2, hop))
            def _():
                backward(h, chip2, hop).wait_send()

            e = hop + 1

            @pl.when((z - e >= 0) & (e <= fmax))
            def _():
                share(h, z - e, c, e).wait_send()

            @pl.when((z + e >= chips) & (lax.rem(z + e, chips) < bmax) & (e <= bmax))
            def _():
                share(h, lax.rem(z + e, chips), c, far + e).wait_send()

    lax.fori_loop(0, kvh, drain, None)

    def store(i, _):
        at = pl.ds(pl.multiple_of(i * 16, 16), 16)
        xs[at, :] = acc[at, :].astype(xs.dtype)

    lax.fori_loop(0, tok // 16, store, None)
    y_store = pltpu.make_async_copy(xs, y_hbm, load.at[0])
    y_store.start()
    y_store.wait()


def solution(mesh):
    chips = mesh.shape["sp"] // CORES

    def step(x, gain, wq, wk, wv, wo):
        tok, depth = x.shape
        kvh = wk.shape[1] // HEAD
        group = wq.shape[1] // wk.shape[1]
        half = HEAD // 2
        place = lax.axis_index("sp") * tok + jnp.arange(tok)
        angle = place.astype(jnp.float32)[:, None] * THETA ** (-jnp.arange(half, dtype=jnp.float32) / half)
        cos, sin = jnp.cos(angle), jnp.sin(angle)
        cos, sin = jnp.concatenate([cos, cos], 1), jnp.concatenate([-sin, sin], 1)
        far = chips // 2
        wide = group * HEAD
        hbm = pl.BlockSpec(memory_space=pl.ANY)
        vmem = pl.BlockSpec(memory_space=pltpu.VMEM)
        dma = pltpu.SemaphoreType.DMA
        bf, f32 = jnp.bfloat16, jnp.float32
        return pl.pallas_call(
            functools.partial(kernel, chips=chips, kvh=kvh, group=group),
            out_shape=jax.ShapeDtypeStruct(x.shape, x.dtype),
            in_specs=[hbm, vmem, vmem, vmem, hbm, hbm, hbm, hbm],
            out_specs=hbm,
            scratch_shapes=[
                pltpu.VMEM((tok, depth), bf),
                pltpu.VMEM((tok, depth), bf),
                pltpu.VMEM((kvh, chips * CORES, 2 * tok, HEAD), bf),
                pltpu.VMEM((kvh, group * tok, HEAD), bf),
                pltpu.VMEM((kvh, HEAD + 8, group * tok), f32),
                pltpu.VMEM((kvh, 1, group * tok), f32),
                pltpu.VMEM((depth, 4 * HEAD), bf),
                pltpu.VMEM((depth, wide), bf),
                pltpu.VMEM((wide, depth), bf),
                pltpu.VMEM((tok, depth), f32),
                dma((5,)),
                dma((kvh, far)),
                dma((kvh, far)),
                dma((kvh, far)),
                dma((kvh, far)),
                dma((kvh, 2 * far + 1)),
                dma((kvh, 2 * far + 1)),
            ],
            compiler_params=pltpu.CompilerParams(collective_id=0, has_side_effects=True, vmem_limit_bytes=67043328),
        )(x, gain[None], cos, sin, wq, wk, wv, wo)

    tokens, whole = P(("dp", "sp"), None), P(None, None)
    return jax.shard_map(
        step,
        mesh=mesh,
        in_specs=(tokens, P(None), whole, whole, whole, whole),
        out_specs=tokens,
        check_vma=False,
    )
```

```python
import functools

import jax
import jax.numpy as jnp
import numpy as np
from jax import lax
from jax.experimental import pallas as pl
from jax.experimental.pallas import tpu as pltpu
from jax.sharding import PartitionSpec as P

HEAD = 128
THETA = 10000
NEG = -1e30
HIDDEN = 2 * NEG
LOG2E = 1.4426950408889634
CORES = 2
MESH = pl.DeviceIdType.MESH


def dot(a, b, ca=1, cb=0):
    return lax.dot_general(a, b, (((ca,), (cb,)), ((), ())), preferred_element_type=jnp.float32)


def kernel(x_hbm, gain_ref, freq_ref, wq, wk, wv, wo, sum_hbm, seen_ref, xs, a, kv, qs, mix, tops, colkv, colq, rows, acc, cos_s, sin_s, probs, keeps,
           load, fsend, frecv, bsend, brecv, ssend, srecv, *, chips, kvh, group):
    me = lax.axis_index("sp")
    z, c = lax.div(me, CORES), lax.rem(me, CORES)
    tok, depth = xs.shape
    wide = group * HEAD
    cols = group * tok
    far = chips // 2
    e2 = HEAD**-0.5 * LOG2E
    fmax = jnp.where(c == 0, far, far - 1)
    bmax = chips - 1 - fmax
    after = lax.rem(z + 1, chips) * CORES + c
    before = lax.rem(z + chips - 1, chips) * CORES + c
    other = z * CORES + 1 - c

    barrier = pltpu.get_barrier_semaphore()
    for peer in (after, before, other):
        pl.semaphore_signal(barrier, inc=1, device_id={"sp": peer}, device_id_type=MESH)

    x_load = pltpu.make_async_copy(x_hbm, xs, load.at[0])

    def kv_load(pair):
        at = pl.ds(pl.multiple_of(pair * 2 * HEAD, 2 * HEAD), 2 * HEAD)
        return (pltpu.make_async_copy(wk.at[:, at], colkv.at[:, pl.ds(0, 2 * HEAD)], load.at[1]),
                pltpu.make_async_copy(wv.at[:, at], colkv.at[:, pl.ds(2 * HEAD, 2 * HEAD)], load.at[2]))

    def q_load(h):
        return pltpu.make_async_copy(wq.at[:, pl.ds(pl.multiple_of(h * wide, wide), wide)], colq, load.at[3])

    def o_load(h):
        return pltpu.make_async_copy(wo.at[pl.ds(pl.multiple_of(h * wide, wide), wide), :], rows, load.at[4])

    x_load.start()
    for copy in kv_load(0):
        copy.start()

    half = HEAD // 2
    lane = lax.broadcasted_iota(jnp.int32, (tok, HEAD), 1)
    place = (me * tok + lax.broadcasted_iota(jnp.int32, (tok, HEAD), 0)).astype(jnp.float32)
    angle = place * freq_ref[...]
    cos_s[...] = jnp.cos(angle)
    sin_s[...] = jnp.where(lane < half, -1.0, 1.0) * jnp.sin(angle)

    def forward(h, chip, hop):
        piece = kv.at[h, chip * CORES + c]
        return pltpu.make_async_remote_copy(piece, piece, fsend.at[h, hop], frecv.at[h, hop], device_id={"sp": after}, device_id_type=MESH)

    def backward(h, chip, hop):
        piece = kv.at[h, chip * CORES + c]
        return pltpu.make_async_remote_copy(piece, piece, bsend.at[h, hop], brecv.at[h, hop], device_id={"sp": before}, device_id_type=MESH)

    def share(h, chip, core, way):
        piece = kv.at[h, chip * CORES + core]
        return pltpu.make_async_remote_copy(piece, piece, ssend.at[h, way], srecv.at[h, way], device_id={"sp": other}, device_id_type=MESH)

    def goes_forward(chip, hop):
        return (chip >= 0) & (chip + hop + 1 < chips) & (hop + 1 <= fmax)

    def goes_backward(chip, hop):
        return (chip < bmax) & (hop + 1 <= bmax)

    x_load.wait()
    q_load(0).start()
    o_load(0).start()
    gain = gain_ref[...].astype(jnp.float32).reshape(1, depth)

    def norm(i, _):
        for n in range(4):
            at = pl.ds(pl.multiple_of(i * 64 + n * 16, 16), 16)
            t = xs[at, :].astype(jnp.float32)
            scale = lax.rsqrt(jnp.mean(t * t, -1, keepdims=True) + 1e-6)
            a[at, :] = (t * scale * gain).astype(a.dtype)

    lax.fori_loop(0, tok // 64, norm, None)

    def turned(t):
        t = t.astype(jnp.bfloat16).astype(jnp.float32)
        return (t * cos_s[...] + pltpu.roll(t, HEAD // 2, 1) * sin_s[...]).astype(jnp.bfloat16)

    def project_kv(pair):
        for copy in kv_load(pair):
            copy.wait()
        k = dot(a[...], colkv[:, : 2 * HEAD])
        v = dot(a[...], colkv[:, 2 * HEAD :])
        for i in range(2):
            h = 2 * pair + i
            kv[h, me, :tok, :] = turned(k[:, i * HEAD : (i + 1) * HEAD])
            vt = v[:, i * HEAD : (i + 1) * HEAD].astype(jnp.bfloat16).T
            for n in range(tok // HEAD):
                kv[h, me, tok + n * HEAD : tok + (n + 1) * HEAD, :] = vt[:, n * HEAD : (n + 1) * HEAD]

        @pl.when(pair + 1 < kvh // 2)
        def _():
            for copy in kv_load(pair + 1):
                copy.start()

    def project_q(h):
        q_load(h).wait()
        t = dot(a[...], colq[...])
        for n in range(group):
            qs[h, n * tok : (n + 1) * tok, :] = turned(t[:, n * HEAD : (n + 1) * HEAD])

        @pl.when(h + 1 < kvh)
        def _():
            q_load(h + 1).start()

    strip = 256
    strips = range(0, cols, strip)

    def values(h, chip):
        parts = [kv[h, chip * CORES + i, tok + n * HEAD : tok + (n + 1) * HEAD, :] for i in range(CORES) for n in range(tok // HEAD)]
        vt = jnp.concatenate(parts, axis=1)
        return jnp.concatenate([vt, jnp.ones((8, CORES * tok), vt.dtype)], axis=0)

    def add(h, vt, at):
        mix[h, :, at : at + strip] = mix[h, :, at : at + strip] * keeps[:, at : at + strip] + dot(vt, probs[:, at : at + strip])

    def attend(h, chip, first, last_h, last_chip):
        k = kv[h, pl.ds(chip * CORES, CORES), :tok, :].reshape(CORES * tok, HEAD)
        vt = values(last_h, last_chip)
        for at in strips:
            s = dot(k, qs[h, at : at + strip, :], 1, 1)
            add(last_h, vt, at)
            if first:
                query = lax.rem(lax.broadcasted_iota(jnp.int32, s.shape, 1) + at, tok) + c * tok
                s = jnp.where(lax.broadcasted_iota(jnp.int32, s.shape, 0) <= query, s, HIDDEN)
            old = tops[h, :, at : at + strip]
            top = jnp.maximum(old, s.max(axis=0, keepdims=True))
            keeps[:, at : at + strip] = jnp.exp2((old - top) * e2)
            tops[h, :, at : at + strip] = top
            probs[:, at : at + strip] = jnp.exp2((s - top) * e2).astype(probs.dtype)

    sum_store = pltpu.make_async_copy(acc, sum_hbm, load.at[0])

    def finish(h):
        parts = []
        for n in range(group):
            at = slice(n * tok, (n + 1) * tok)
            parts.append((mix[h, :HEAD, at] * (1 / mix[h, HEAD : HEAD + 1, at])).astype(jnp.bfloat16).T)
        seen = jnp.concatenate(parts, axis=1)

        @pl.when(h < kvh - 1)
        def _():
            o_load(h).wait()
            acc[...] += dot(seen, rows[...])

            @pl.when(h + 2 < kvh)
            def _():
                o_load(h + 1).start()

        @pl.when(h == kvh - 2)
        def _():
            sum_store.start()

        @pl.when(h == kvh - 1)
        def _():
            seen_ref[...] = seen

    def send_own(h):
        @pl.when(goes_forward(z, 0))
        def _():
            forward(h, z, 0).start()

        @pl.when(goes_backward(z, 0))
        def _():
            backward(h, z, 0).start()

        share(h, z, c, 0).start()

    def receive(h, e):
        chip = z - e

        @pl.when((chip >= 0) & (e <= fmax))
        def _():
            forward(h, chip, e - 1).wait_recv()

            @pl.when(goes_forward(chip, e))
            def _():
                forward(h, chip, e).start()

            share(h, chip, c, e).start()

        chip2 = lax.rem(z + e, chips)

        @pl.when((chip2 < bmax) & (e <= bmax))
        def _():
            backward(h, chip2, e - 1).wait_recv()

            @pl.when(goes_backward(chip2, e))
            def _():
                backward(h, chip2, e).start()

            @pl.when(z + e >= chips)
            def _():
                share(h, chip2, c, far + e).start()

    project_kv(0)
    pl.semaphore_wait(barrier, 3)
    send_own(0)
    project_q(0)

    def begin(i, _):
        at = pl.ds(pl.multiple_of(i * 64, 64), 64)
        acc[at, :] = xs[at, :].astype(jnp.float32)

    lax.fori_loop(0, tok // 64, begin, None)

    def clear(h, _):
        mix[h] = jnp.zeros(mix.shape[1:], mix.dtype)
        tops[h] = jnp.full(tops.shape[1:], NEG, tops.dtype)

    lax.fori_loop(0, kvh, clear, None)
    probs[...] = jnp.zeros_like(probs)
    keeps[...] = jnp.ones_like(keeps)

    def round_(t, last):
        @pl.when(t + 1 < kvh)
        def _():
            send_own(t + 1)

        for e in range(1, far + 1):
            @pl.when((t >= e) & (t - e < kvh))
            def _():
                receive(t - e, e)

        @pl.when((lax.rem(t, 2) == 0) & (t + 2 < kvh))
        def _():
            project_kv(lax.div(t, 2) + 1)

        @pl.when(t < kvh)
        def _():
            share(t, z, 1 - c, 0).wait_recv()
            attend(t, z, True, *last)

        last = jnp.where(t < kvh, t, last[0]), jnp.where(t < kvh, z, last[1])

        def piece(j, last):
            e = lax.div(j, 2) + 1
            back = lax.rem(j, 2)
            h = t - e
            chip = jnp.where(back == 1, z + e - chips, z - e)
            ok = (h >= 0) & (h < kvh) & (chip >= 0)

            @pl.when(ok)
            def _():
                way = jnp.where(e == far, jnp.where(c == 0, 2 * far, far), e + back * far)
                share(h, chip, 1 - c, way).wait_recv()
                attend(h, chip, False, *last)

            return jnp.where(ok, h, last[0]), jnp.where(ok, chip, last[1])

        last = lax.fori_loop(0, 2 * far - 1, piece, last)

        @pl.when(t + 1 < kvh)
        def _():
            project_q(t + 1)

        @pl.when(t == kvh + far)
        def _():
            vt = values(*last)
            for at in strips:
                add(last[0], vt, at)

        @pl.when(t > far)
        def _():
            finish(t - far - 1)

        return last

    lax.fori_loop(0, kvh + far + 1, round_, (jnp.int32(0), z))

    def drain(h, _):
        share(h, z, c, 0).wait_send()
        for hop in range(far):
            chip = z - hop

            @pl.when(goes_forward(chip, hop))
            def _():
                forward(h, chip, hop).wait_send()

            chip2 = lax.rem(z + hop, chips)

            @pl.when(goes_backward(chip2, hop))
            def _():
                backward(h, chip2, hop).wait_send()

            e = hop + 1

            @pl.when((z - e >= 0) & (e <= fmax))
            def _():
                share(h, z - e, c, e).wait_send()

            @pl.when((z + e >= chips) & (lax.rem(z + e, chips) < bmax) & (e <= bmax))
            def _():
                share(h, lax.rem(z + e, chips), c, far + e).wait_send()

    lax.fori_loop(0, kvh, drain, None)

    sum_store.wait()


def last_head(seen_ref, wo_ref, sum_ref, y_ref):
    y_ref[...] = (sum_ref[...] + dot(seen_ref[...], wo_ref[...])).astype(y_ref.dtype)


def solution(mesh):
    chips = mesh.shape["sp"] // CORES

    def step(x, gain, wq, wk, wv, wo):
        tok, depth = x.shape
        kvh = wk.shape[1] // HEAD
        group = wq.shape[1] // wk.shape[1]
        half = HEAD // 2
        freq = THETA ** (-np.arange(half, dtype=np.float64) / half)
        freq = jnp.asarray(np.concatenate([freq, freq])[None], jnp.float32)
        far = chips // 2
        wide = group * HEAD
        hbm = pl.BlockSpec(memory_space=pl.ANY)
        vmem = pl.BlockSpec(memory_space=pltpu.VMEM)
        dma = pltpu.SemaphoreType.DMA
        bf, f32 = jnp.bfloat16, jnp.float32
        sums, seen = pl.pallas_call(
            functools.partial(kernel, chips=chips, kvh=kvh, group=group),
            out_shape=[jax.ShapeDtypeStruct(x.shape, f32), jax.ShapeDtypeStruct((tok, wide), bf)],
            in_specs=[hbm, vmem, vmem, hbm, hbm, hbm, hbm],
            out_specs=[hbm, vmem],
            scratch_shapes=[
                pltpu.VMEM((tok, depth), bf),
                pltpu.VMEM((tok, depth), bf),
                pltpu.VMEM((kvh, chips * CORES, 2 * tok, HEAD), bf),
                pltpu.VMEM((kvh, group * tok, HEAD), bf),
                pltpu.VMEM((kvh, HEAD + 8, group * tok), f32),
                pltpu.VMEM((kvh, 1, group * tok), f32),
                pltpu.VMEM((depth, 4 * HEAD), bf),
                pltpu.VMEM((depth, wide), bf),
                pltpu.VMEM((wide, depth), bf),
                pltpu.VMEM((tok, depth), f32),
                pltpu.VMEM((tok, HEAD), f32),
                pltpu.VMEM((tok, HEAD), f32),
                pltpu.VMEM((CORES * tok, group * tok), bf),
                pltpu.VMEM((1, group * tok), f32),
                dma((5,)),
                dma((kvh, far)),
                dma((kvh, far)),
                dma((kvh, far)),
                dma((kvh, far)),
                dma((kvh, 2 * far + 1)),
                dma((kvh, 2 * far + 1)),
            ],
            compiler_params=pltpu.CompilerParams(collective_id=0, has_side_effects=True, vmem_limit_bytes=60 * 2**20),
        )(x, gain, freq, wq, wk, wv, wo)
        block = depth // 2
        return pl.pallas_call(
            last_head,
            grid=(depth // block,),
            out_shape=jax.ShapeDtypeStruct(x.shape, x.dtype),
            in_specs=[
                pl.BlockSpec((tok, wide), lambda n: (0, 0)),
                pl.BlockSpec((wide, block), lambda n: (kvh - 1, n)),
                pl.BlockSpec((tok, block), lambda n: (0, n)),
            ],
            out_specs=pl.BlockSpec((tok, block), lambda n: (0, n)),
            compiler_params=pltpu.CompilerParams(dimension_semantics=("arbitrary",)),
            cost_estimate=pl.CostEstimate(flops=2 * tok * wide * depth, bytes_accessed=2 * wide * depth + 6 * tok * depth, transcendentals=0),
        )(seen, wo, sums)

    tokens, whole = P(("dp", "sp"), None), P(None, None)
    return jax.shard_map(
        step,
        mesh=mesh,
        in_specs=(tokens, P(None), whole, whole, whole, whole),
        out_specs=tokens,
        check_vma=False,
    )
```

```python
import functools

import jax
import jax.numpy as jnp
import numpy as np
from jax import lax
from jax.experimental import pallas as pl
from jax.experimental.pallas import tpu as pltpu
from jax.sharding import PartitionSpec as P

HEAD = 128
THETA = 10000
NEG = -1e30
HIDDEN = 2 * NEG
LOG2E = 1.4426950408889634
CORES = 2
MESH = pl.DeviceIdType.MESH


def dot(a, b, ca=1, cb=0):
    return lax.dot_general(a, b, (((ca,), (cb,)), ((), ())), preferred_element_type=jnp.float32)


def kernel(x_hbm, gain_ref, freq_ref, wq, wk, wv, wo, sum_hbm, seen_ref, xs, a, kv, qs, mix, tops, colkv, colq, rows, acc, cos_s, sin_s, probs, keeps,
           load, fsend, frecv, bsend, brecv, ssend, srecv, *, chips, kvh, group):
    me = lax.axis_index("sp")
    z, c = lax.div(me, CORES), lax.rem(me, CORES)
    tok, depth = xs.shape
    wide = group * HEAD
    cols = group * tok
    far = chips // 2
    e2 = HEAD**-0.5 * LOG2E
    fmax = jnp.where(c == 0, far, far - 1)
    bmax = chips - 1 - fmax
    after = lax.rem(z + 1, chips) * CORES + c
    before = lax.rem(z + chips - 1, chips) * CORES + c
    other = z * CORES + 1 - c

    barrier = pltpu.get_barrier_semaphore()
    for peer in (after, before, other):
        pl.semaphore_signal(barrier, inc=1, device_id={"sp": peer}, device_id_type=MESH)

    x_load = pltpu.make_async_copy(x_hbm, xs, load.at[0])

    def kv_load(pair):
        at = pl.ds(pl.multiple_of(pair * 2 * HEAD, 2 * HEAD), 2 * HEAD)
        return (pltpu.make_async_copy(wk.at[:, at], colkv.at[:, pl.ds(0, 2 * HEAD)], load.at[1]),
                pltpu.make_async_copy(wv.at[:, at], colkv.at[:, pl.ds(2 * HEAD, 2 * HEAD)], load.at[2]))

    def q_load(h):
        return pltpu.make_async_copy(wq.at[:, pl.ds(pl.multiple_of(h * wide, wide), wide)], colq, load.at[3])

    def o_load(h):
        return pltpu.make_async_copy(wo.at[pl.ds(pl.multiple_of(h * wide, wide), wide), :], rows, load.at[4])

    x_load.start()
    for copy in kv_load(0):
        copy.start()

    half = HEAD // 2
    lane = lax.broadcasted_iota(jnp.int32, (tok, HEAD), 1)
    place = (me * tok + lax.broadcasted_iota(jnp.int32, (tok, HEAD), 0)).astype(jnp.float32)
    angle = place * freq_ref[...]
    cos_s[...] = jnp.cos(angle)
    sin_s[...] = jnp.where(lane < half, -1.0, 1.0) * jnp.sin(angle)

    def forward(h, chip, hop):
        piece = kv.at[h, chip * CORES + c]
        return pltpu.make_async_remote_copy(piece, piece, fsend.at[h, hop], frecv.at[h, hop], device_id={"sp": after}, device_id_type=MESH)

    def backward(h, chip, hop):
        piece = kv.at[h, chip * CORES + c]
        return pltpu.make_async_remote_copy(piece, piece, bsend.at[h, hop], brecv.at[h, hop], device_id={"sp": before}, device_id_type=MESH)

    def share(h, chip, core, way):
        piece = kv.at[h, chip * CORES + core]
        return pltpu.make_async_remote_copy(piece, piece, ssend.at[h, way], srecv.at[h, way], device_id={"sp": other}, device_id_type=MESH)

    def goes_forward(chip, hop):
        return (chip >= 0) & (chip + hop + 1 < chips) & (hop + 1 <= fmax)

    def goes_backward(chip, hop):
        return (chip < bmax) & (hop + 1 <= bmax)

    x_load.wait()
    q_load(0).start()
    o_load(0).start()
    gain = gain_ref[...].astype(jnp.float32).reshape(1, depth)

    def norm(i, _):
        for n in range(4):
            at = pl.ds(pl.multiple_of(i * 64 + n * 16, 16), 16)
            t = xs[at, :].astype(jnp.float32)
            scale = lax.rsqrt(jnp.mean(t * t, -1, keepdims=True) + 1e-6)
            a[at, :] = (t * scale * gain).astype(a.dtype)

    lax.fori_loop(0, tok // 64, norm, None)

    def turned(t):
        t = t.astype(jnp.bfloat16).astype(jnp.float32)
        return (t * cos_s[...] + pltpu.roll(t, HEAD // 2, 1) * sin_s[...]).astype(jnp.bfloat16)

    def project_kv(pair):
        for copy in kv_load(pair):
            copy.wait()
        k = dot(a[...], colkv[:, : 2 * HEAD])
        v = dot(a[...], colkv[:, 2 * HEAD :])
        for i in range(2):
            h = 2 * pair + i
            kv[h, me, :tok, :] = turned(k[:, i * HEAD : (i + 1) * HEAD])
            vt = v[:, i * HEAD : (i + 1) * HEAD].astype(jnp.bfloat16).T
            for n in range(tok // HEAD):
                kv[h, me, tok + n * HEAD : tok + (n + 1) * HEAD, :] = vt[:, n * HEAD : (n + 1) * HEAD]

        @pl.when(pair + 1 < kvh // 2)
        def _():
            for copy in kv_load(pair + 1):
                copy.start()

    def project_q(h):
        q_load(h).wait()
        t = dot(a[...], colq[...])
        for n in range(group):
            qs[h, n * tok : (n + 1) * tok, :] = turned(t[:, n * HEAD : (n + 1) * HEAD])

        @pl.when(h + 1 < kvh)
        def _():
            q_load(h + 1).start()

    strip = 256
    strips = range(0, cols, strip)

    def values(h, chip):
        parts = [kv[h, chip * CORES + i, tok + n * HEAD : tok + (n + 1) * HEAD, :] for i in range(CORES) for n in range(tok // HEAD)]
        vt = jnp.concatenate(parts, axis=1)
        return jnp.concatenate([vt, jnp.ones((8, CORES * tok), vt.dtype)], axis=0)

    def add(h, vt, at):
        mix[h, :, at : at + strip] = mix[h, :, at : at + strip] * keeps[:, at : at + strip] + dot(vt, probs[:, at : at + strip])

    def attend(h, chip, first, last_h, last_chip):
        k = kv[h, pl.ds(chip * CORES, CORES), :tok, :].reshape(CORES * tok, HEAD)
        vt = values(last_h, last_chip)
        for at in strips:
            s = dot(k, qs[h, at : at + strip, :], 1, 1)
            add(last_h, vt, at)
            if first:
                query = lax.rem(lax.broadcasted_iota(jnp.int32, s.shape, 1) + at, tok) + c * tok
                s = jnp.where(lax.broadcasted_iota(jnp.int32, s.shape, 0) <= query, s, HIDDEN)
            old = tops[h, :, at : at + strip]
            top = jnp.maximum(old, s.max(axis=0, keepdims=True))
            keeps[:, at : at + strip] = jnp.exp2((old - top) * e2)
            tops[h, :, at : at + strip] = top
            probs[:, at : at + strip] = jnp.exp2((s - top) * e2).astype(probs.dtype)

    sum_store = pltpu.make_async_copy(acc, sum_hbm, load.at[0])

    def finish(h):
        parts = []
        for n in range(group):
            at = slice(n * tok, (n + 1) * tok)
            parts.append((mix[h, :HEAD, at] * (1 / mix[h, HEAD : HEAD + 1, at])).astype(jnp.bfloat16).T)
        seen = jnp.concatenate(parts, axis=1)

        @pl.when(h < kvh - 1)
        def _():
            o_load(h).wait()
            acc[...] += dot(seen, rows[...])

            @pl.when(h + 2 < kvh)
            def _():
                o_load(h + 1).start()

        @pl.when(h == kvh - 2)
        def _():
            sum_store.start()

        @pl.when(h == kvh - 1)
        def _():
            seen_ref[...] = seen

    def send_own(h):
        @pl.when(goes_forward(z, 0))
        def _():
            forward(h, z, 0).start()

        @pl.when(goes_backward(z, 0))
        def _():
            backward(h, z, 0).start()

        share(h, z, c, 0).start()

    def receive(h, e):
        chip = z - e

        @pl.when((chip >= 0) & (e <= fmax))
        def _():
            forward(h, chip, e - 1).wait_recv()

            if e < far:

                @pl.when(goes_forward(chip, e))
                def _():
                    forward(h, chip, e).start()

            share(h, chip, c, e).start()

        chip2 = lax.rem(z + e, chips)

        @pl.when((chip2 < bmax) & (e <= bmax))
        def _():
            backward(h, chip2, e - 1).wait_recv()

            if e < far:

                @pl.when(goes_backward(chip2, e))
                def _():
                    backward(h, chip2, e).start()

            @pl.when(z + e >= chips)
            def _():
                share(h, chip2, c, far + e).start()

    project_kv(0)
    pl.semaphore_wait(barrier, 3)
    send_own(0)
    send_own(1)
    project_q(0)

    def begin(i, _):
        at = pl.ds(pl.multiple_of(i * 64, 64), 64)
        acc[at, :] = xs[at, :].astype(jnp.float32)

    lax.fori_loop(0, tok // 64, begin, None)

    def clear(h, _):
        mix[h] = jnp.zeros(mix.shape[1:], mix.dtype)
        tops[h] = jnp.full(tops.shape[1:], NEG, tops.dtype)

    lax.fori_loop(0, kvh, clear, None)
    probs[...] = jnp.zeros_like(probs)
    keeps[...] = jnp.ones_like(keeps)

    def round_(t, last):
        def receive_from(a, b):
            for e in range(a, b):
                @pl.when((t >= e) & (t - e < kvh))
                def _():
                    receive(t - e, e)

        receive_from(1, far - 1)

        @pl.when(t + 1 < kvh // 2)
        def _():
            project_kv(t + 1)

        @pl.when(t < kvh)
        def _():
            share(t, z, 1 - c, 0).wait_recv()
            attend(t, z, True, *last)

        receive_from(far - 1, far + 1)

        @pl.when(t + 2 < kvh)
        def _():
            send_own(t + 2)

        last = jnp.where(t < kvh, t, last[0]), jnp.where(t < kvh, z, last[1])

        def piece(i, last):
            e = i + 1
            h = t - e
            ok = (h >= 0) & (h < kvh)
            ahead, behind = z - e, z + e - chips
            one = ok & (ahead >= 0)
            two = ok & (behind >= 0) & (e < far)
            way = jnp.where(e == far, jnp.where(c == 0, 2 * far, far), e)

            @pl.when(one & two)
            def _():
                share(h, ahead, 1 - c, way).wait_recv()
                share(h, behind, 1 - c, e + far).wait_recv()
                attend(h, ahead, False, *last)
                attend(h, behind, False, h, ahead)

            @pl.when(one & jnp.logical_not(two))
            def _():
                share(h, ahead, 1 - c, way).wait_recv()
                attend(h, ahead, False, *last)

            @pl.when(two & jnp.logical_not(one))
            def _():
                share(h, behind, 1 - c, e + far).wait_recv()
                attend(h, behind, False, *last)

            return jnp.where(one | two, h, last[0]), jnp.where(two, behind, jnp.where(one, ahead, last[1]))

        last = lax.fori_loop(0, far, piece, last)

        @pl.when(t + 1 < kvh)
        def _():
            project_q(t + 1)

        @pl.when(t == kvh + far)
        def _():
            vt = values(*last)
            for at in strips:
                add(last[0], vt, at)

        @pl.when(t > far)
        def _():
            finish(t - far - 1)

        return last

    lax.fori_loop(0, kvh + far + 1, round_, (jnp.int32(0), z))

    def drain(h, _):
        share(h, z, c, 0).wait_send()
        for hop in range(far):
            chip = z - hop

            @pl.when(goes_forward(chip, hop))
            def _():
                forward(h, chip, hop).wait_send()

            chip2 = lax.rem(z + hop, chips)

            @pl.when(goes_backward(chip2, hop))
            def _():
                backward(h, chip2, hop).wait_send()

            e = hop + 1

            @pl.when((z - e >= 0) & (e <= fmax))
            def _():
                share(h, z - e, c, e).wait_send()

            @pl.when((z + e >= chips) & (lax.rem(z + e, chips) < bmax) & (e <= bmax))
            def _():
                share(h, lax.rem(z + e, chips), c, far + e).wait_send()

    lax.fori_loop(0, kvh, drain, None)

    sum_store.wait()


def last_head(seen_ref, wo_ref, sum_ref, y_ref):
    y_ref[...] = (sum_ref[...] + dot(seen_ref[...], wo_ref[...])).astype(y_ref.dtype)


def solution(mesh):
    chips = mesh.shape["sp"] // CORES

    def step(x, gain, wq, wk, wv, wo):
        tok, depth = x.shape
        kvh = wk.shape[1] // HEAD
        group = wq.shape[1] // wk.shape[1]
        half = HEAD // 2
        freq = THETA ** (-np.arange(half, dtype=np.float64) / half)
        freq = jnp.asarray(np.concatenate([freq, freq])[None], jnp.float32)
        far = chips // 2
        wide = group * HEAD
        hbm = pl.BlockSpec(memory_space=pl.ANY)
        vmem = pl.BlockSpec(memory_space=pltpu.VMEM)
        dma = pltpu.SemaphoreType.DMA
        bf, f32 = jnp.bfloat16, jnp.float32
        sums, seen = pl.pallas_call(
            functools.partial(kernel, chips=chips, kvh=kvh, group=group),
            out_shape=[jax.ShapeDtypeStruct(x.shape, f32), jax.ShapeDtypeStruct((tok, wide), bf)],
            in_specs=[hbm, vmem, vmem, hbm, hbm, hbm, hbm],
            out_specs=[hbm, vmem],
            scratch_shapes=[
                pltpu.VMEM((tok, depth), bf),
                pltpu.VMEM((tok, depth), bf),
                pltpu.VMEM((kvh, chips * CORES, 2 * tok, HEAD), bf),
                pltpu.VMEM((kvh, group * tok, HEAD), bf),
                pltpu.VMEM((kvh, HEAD + 8, group * tok), f32),
                pltpu.VMEM((kvh, 1, group * tok), f32),
                pltpu.VMEM((depth, 4 * HEAD), bf),
                pltpu.VMEM((depth, wide), bf),
                pltpu.VMEM((wide, depth), bf),
                pltpu.VMEM((tok, depth), f32),
                pltpu.VMEM((tok, HEAD), f32),
                pltpu.VMEM((tok, HEAD), f32),
                pltpu.VMEM((CORES * tok, group * tok), bf),
                pltpu.VMEM((1, group * tok), f32),
                dma((5,)),
                dma((kvh, far)),
                dma((kvh, far)),
                dma((kvh, far)),
                dma((kvh, far)),
                dma((kvh, 2 * far + 1)),
                dma((kvh, 2 * far + 1)),
            ],
            compiler_params=pltpu.CompilerParams(collective_id=0, has_side_effects=True, vmem_limit_bytes=60 * 2**20),
        )(x, gain, freq, wq, wk, wv, wo)
        block = depth // 2
        return pl.pallas_call(
            last_head,
            grid=(depth // block,),
            out_shape=jax.ShapeDtypeStruct(x.shape, x.dtype),
            in_specs=[
                pl.BlockSpec((tok, wide), lambda n: (0, 0)),
                pl.BlockSpec((wide, block), lambda n: (kvh - 1, n)),
                pl.BlockSpec((tok, block), lambda n: (0, n)),
            ],
            out_specs=pl.BlockSpec((tok, block), lambda n: (0, n)),
            compiler_params=pltpu.CompilerParams(dimension_semantics=("arbitrary",)),
            cost_estimate=pl.CostEstimate(flops=2 * tok * wide * depth, bytes_accessed=2 * wide * depth + 6 * tok * depth, transcendentals=0),
        )(seen, wo, sums)

    tokens, whole = P(("dp", "sp"), None), P(None, None)
    return jax.shard_map(
        step,
        mesh=mesh,
        in_specs=(tokens, P(None), whole, whole, whole, whole),
        out_specs=tokens,
        check_vma=False,
    )
```
